32 devices in a mesh: dp: 8 (over z, x), mp: 4 (over y, core).
Axes of the slice: x: 2, y: 2, z: 4, core: 2. Of those that a mesh axis runs over, the one named last changes fastest.
Arguments:
- query_rows: bfloat16 [512, 2560], P('dp', 'mp'), may hold values from -48 to 48
- doc_rows: bfloat16 [512, 2560], P('dp', 'mp'), may hold values from -48 to 48
- head: bfloat16 [2560, 2560], P(None, 'mp'), may hold values from -0.125 to 0.125
- logit_scale: float32 [7], replicated, may hold values from 1 to 3
- loss_grad: float32 [512, 7], P('dp'), may hold values from 0.5 to 2
- shortlist: int32 [512, 128], P('dp'), may hold values from 0 to 127, as said below
- send_rows: int32 [8, 128], P('dp'), may hold values from -1 to 63, as said below
Outputs:
- query_grad: bfloat16 [512, 2560], P('dp', 'mp')
- doc_grad: bfloat16 [512, 2560], P('dp', 'mp')
- head_grad: float32 [2560, 2560], P('dp', 'mp')
The draws below stay inside these ranges and needn't reach their ends.
Inputs may be any that keep to these rules, and one draw needn't show every extreme that they name: shortlist[i, n] is a slot o * 16 + j of the rows fetched for the owner of query i, and send_rows at place j of the block owner o sends to that owner is never -1. send_rows[o, r * 16 + j] is a row among owner o's 64 documents, sent to owner r at place j; in each block of 16 places the rows are distinct and come first, -1 fills the rest; the block an owner sends to itself is always full.
All inputs are finite; a program needn't handle non-finite values.
Results may differ from the reference program's by a relative error of at most 0.014.
The reference program's roundings to bfloat16 on the way count: a program that leaves them out, or rounds other values in their place, can miss the bound.
Values may be sent and summed in bfloat16 or wider, within the bound.
No kernel may reach another device: no remote copies, remote signals or barrier semaphores. Data moves between devices by JAX's collectives and lax.ppermute only.
A program may use at most 64 MiB of HBM per device.

```python
import math
import jax
import jax.numpy as jnp
from jax import lax

D = 2560
QL = 64
NEG = 128
NW = 7
NQ = 512
FETCH_ROWS = 128
N_DP = 8


def fetch_plan(key):
    fetch_block = FETCH_ROWS // N_DP
    base_key = jax.random.fold_in(key, 7001)
    count_key, order_key, owner_key, pick_key = jax.random.split(base_key, 4)
    least_count = (fetch_block + 1) // 2
    counts = jax.random.randint(count_key, (N_DP, N_DP), least_count, fetch_block + 1)
    diagonal = jnp.arange(N_DP)[:, None] == jnp.arange(N_DP)[None, :]
    counts = jnp.where(diagonal, fetch_block, counts)
    ranking = jax.random.randint(order_key, (N_DP, N_DP, QL), 0, 1 << 20) * QL + jnp.arange(QL)[None, None, :]
    row_order = jnp.argsort(ranking, axis=2)[:, :, :fetch_block]
    place_ids = jnp.arange(fetch_block)[None, None, :]
    sent_rows = jnp.where(place_ids < counts[:, :, None], row_order, -1).astype(jnp.int32)
    send_rows = sent_rows.reshape(N_DP, N_DP * fetch_block)
    owners = jax.random.randint(owner_key, (NQ, NEG), 0, N_DP)
    requester = jnp.broadcast_to((jnp.arange(NQ) // QL)[:, None], (NQ, NEG))
    available = counts[owners, requester]
    place_pick = jax.random.randint(pick_key, (NQ, NEG), 0, 1 << 16) % available
    shortlist = (owners * fetch_block + place_pick).astype(jnp.int32)
    return (send_rows, shortlist)


def embed_pair(key):
    base_key = jax.random.fold_in(key, 7002)
    query_key, doc_key = jax.random.split(base_key, 2)
    query_vals = jax.random.normal(query_key, (NQ, D), jnp.float32)
    doc_vals = jax.random.normal(doc_key, (NQ, D), jnp.float32)
    return (query_vals, doc_vals)


def draw_query_rows(key, part):
    return embed_pair(key)[0].astype(jnp.bfloat16)


def draw_doc_rows(key, part):
    return embed_pair(key)[1].astype(jnp.bfloat16)


def draw_shortlist(key, part):
    return fetch_plan(key)[1]


def draw_send_rows(key, part):
    return fetch_plan(key)[0]


def block_levels(own_key, shape, cuts, least, high):
    def one(position, blocks):
        draws = jax.random.uniform(jax.random.fold_in(jax.random.fold_in(own_key, 6), position), (blocks,), jnp.float32, least / len(cuts), high / len(cuts))
        return jnp.repeat(jnp.exp(draws), shape[position] // blocks).reshape((-1,) + (1,) * (len(shape) - position - 1))

    level = one(*cuts[0])
    for cut in cuts[1:]:
        level = level * one(*cut)
    return level


def bell_draw(rng, extent, width, limit, cuts=(), kind=jnp.bfloat16):
    values = width * jax.random.normal(rng, extent, jnp.float32)
    if cuts:
        values = values * block_levels(rng, extent, cuts, -0.22, 0.18)
    return jnp.clip(values, -limit, limit).astype(kind)


def setup_inputs(seed: int = 0) -> dict:
    streams_of = jax.random.split(jax.random.key(seed), 8)
    return {
        "query_rows": draw_query_rows(jax.random.fold_in(streams_of[7], 71), 0),
        "doc_rows": draw_doc_rows(jax.random.fold_in(streams_of[7], 71), 0),
        "head": bell_draw(streams_of[2], (D, D), D ** -0.5, 0.125, ((1, 4),)),
        "logit_scale": jnp.clip(jnp.exp(jax.random.uniform(streams_of[3], (NW,), jnp.float32, math.log(1.0), math.log(3.0))), 1.0, 3.0),
        "loss_grad": jnp.clip(jnp.exp(math.log(2.0) - 1.3862944 * jax.random.uniform(streams_of[4], (NQ, NW), jnp.float32) ** block_levels(streams_of[4], (NQ, NW), ((0, 8),), -0.2, 0.2)), 0.5, 2.0),
        "shortlist": draw_shortlist(jax.random.fold_in(streams_of[7], 71), 0),
        "send_rows": draw_send_rows(jax.random.fold_in(streams_of[7], 71), 0),
    }


def width_bounds():
    return [0] + [D // 2 ** (NW - 1 - width_level) for width_level in range(NW)]

def softmax_terms(neg_score, pos_score, width_scale, loss_weight):
    neg_logit = neg_score * width_scale[:, None, None]
    pos_logit = pos_score * width_scale[:, None]
    highest = jnp.maximum(lax.optimization_barrier(jnp.max(neg_logit, axis=2)), pos_logit)
    neg_exp = jnp.exp(neg_logit - highest[:, :, None])
    pos_exp = jnp.exp(pos_logit - highest)
    denominator = lax.optimization_barrier(jnp.sum(neg_exp, axis=2)) + pos_exp
    row_weight = loss_weight * width_scale[:, None]
    neg_grad = neg_exp * (row_weight / denominator)[:, :, None]
    pos_grad = row_weight * (pos_exp / denominator - 1.0)
    return (neg_grad, pos_grad)

def suffix_sum(values):
    return jnp.flip(jnp.cumsum(jnp.flip(values, 0), axis=0), 0)

def reference(query_rows, doc_rows, head, logit_scale, loss_grad, shortlist, send_rows):
    bounds = width_bounds()
    fetch_block = FETCH_ROWS // N_DP
    query_proj = jnp.dot(query_rows, head, preferred_element_type=jnp.float32).astype(jnp.bfloat16)
    doc_proj = jnp.dot(doc_rows, head, preferred_element_type=jnp.float32).astype(jnp.bfloat16)
    widths = jnp.array(bounds[1:], jnp.float32)
    width_scale = logit_scale / jnp.sqrt(widths)
    slot_ids = jnp.arange(FETCH_ROWS, dtype=jnp.int32)
    slot_owner = slot_ids // fetch_block
    slot_place = slot_ids % fetch_block
    col_ids = jnp.arange(D, dtype=jnp.int32)
    seg_onehot = jnp.stack([((col_ids >= bounds[segment]) & (col_ids < bounds[segment + 1])).astype(jnp.float32) for segment in range(NW)])
    query_ids = jnp.arange(QL, dtype=jnp.int32)

    def one_owner(doc_accum, inputs):
        owner_index, owner_query, owner_doc, shortlisted, weight_rows = inputs
        local_rows = send_rows[slot_owner, owner_index * fetch_block + slot_place]
        is_valid = local_rows >= 0
        doc_ids = (slot_owner * QL + jnp.maximum(local_rows, 0)).astype(jnp.int32)
        fetched = doc_proj[doc_ids]
        pieces = []
        for segment in range(NW):
            lower, upper = (bounds[segment], bounds[segment + 1])
            pieces.append(jnp.dot(owner_query[:, lower:upper], fetched[:, lower:upper].T, preferred_element_type=jnp.float32))
        scores = jnp.cumsum(jnp.stack(pieces), axis=0)
        neg_score = jnp.take_along_axis(scores, jnp.broadcast_to(shortlisted[None], (NW, QL, NEG)), axis=2)
        pos_prod = owner_query.astype(jnp.float32) * owner_doc.astype(jnp.float32)
        pos_score = jnp.cumsum(jnp.dot(seg_onehot, pos_prod.T, precision=lax.Precision.HIGHEST), axis=0)
        neg_grad, pos_grad = softmax_terms(neg_score, pos_score, width_scale, weight_rows.T)
        seg_neg = suffix_sum(neg_grad)
        seg_pos = suffix_sum(pos_grad)
        coeff_dense = jax.vmap(lambda values: jnp.zeros((QL, FETCH_ROWS), jnp.float32).at[query_ids[:, None], shortlisted].add(values))(seg_neg).astype(jnp.bfloat16)
        pos_cols = jnp.dot(seg_pos.T, seg_onehot, precision=lax.Precision.HIGHEST)
        query_parts = []
        fetched_parts = []
        for segment in range(NW):
            lower, upper = (bounds[segment], bounds[segment + 1])
            query_parts.append(jnp.dot(coeff_dense[segment], fetched[:, lower:upper], preferred_element_type=jnp.float32))
            fetched_parts.append(jnp.dot(coeff_dense[segment].T, owner_query[:, lower:upper], preferred_element_type=jnp.float32))
        query_back = jnp.concatenate(query_parts, axis=1) + pos_cols * owner_doc.astype(jnp.float32)
        fetched_grad = jnp.concatenate(fetched_parts, axis=1)
        targets = jnp.where(is_valid, doc_ids, NQ).astype(jnp.int32)
        doc_accum = doc_accum.at[targets].add(fetched_grad, mode='drop')
        own_start = (owner_index * QL).astype(jnp.int32)
        own_rows = lax.dynamic_slice_in_dim(doc_accum, own_start, QL, 0) + pos_cols * owner_query.astype(jnp.float32)
        doc_accum = lax.dynamic_update_slice_in_dim(doc_accum, own_rows, own_start, 0)
        return (doc_accum, query_back.astype(jnp.bfloat16))
    owner_range = jnp.arange(N_DP, dtype=jnp.int32)
    inputs = (owner_range, query_proj.reshape(N_DP, QL, D), doc_proj.reshape(N_DP, QL, D), shortlist.reshape(N_DP, QL, NEG), loss_grad.reshape(N_DP, QL, NW))
    doc_accum, query_back = lax.scan(one_owner, jnp.zeros((NQ, D), jnp.float32), inputs)
    grad_proj_q = query_back.reshape(NQ, D)
    grad_proj_d = doc_accum.astype(jnp.bfloat16)
    query_grad = jnp.dot(grad_proj_q, head.T, preferred_element_type=jnp.float32).astype(jnp.bfloat16)
    doc_grad = jnp.dot(grad_proj_d, head.T, preferred_element_type=jnp.float32).astype(jnp.bfloat16)
    head_grad = jnp.dot(query_rows.T, grad_proj_q, preferred_element_type=jnp.float32) + jnp.dot(doc_rows.T, grad_proj_d, preferred_element_type=jnp.float32)
    return (query_grad, doc_grad, head_grad)
```

```python
import functools

import jax
import jax.numpy as jnp
from jax import lax
from jax.experimental import pallas as pl
from jax.experimental.pallas import tpu as pltpu
from jax.sharding import PartitionSpec as P

NW = 7
BF = jnp.bfloat16
F32 = jnp.float32
HI = lax.Precision.HIGHEST

VMEM = pl.BlockSpec(memory_space=pltpu.VMEM)
SMEM = pl.BlockSpec(memory_space=pltpu.SMEM)
ANY = pl.BlockSpec(memory_space=pl.ANY)
PARAMS = pltpu.CompilerParams(vmem_limit_bytes=56 * 1024 * 1024)


def iota(shape, axis):
    return lax.broadcasted_iota(jnp.int32, shape, axis)


def dot(a, b, ca, cb, precision=None):
    return lax.dot_general(
        a, b, (((ca,), (cb,)), ((), ())), precision=precision, preferred_element_type=F32
    )


def call(body, outs, ins, scratch, args, name):
    return pl.pallas_call(
        body,
        out_shape=outs,
        in_specs=ins,
        out_specs=jax.tree.map(lambda _: VMEM, outs),
        scratch_shapes=scratch,
        compiler_params=PARAMS,
        name=name,
    )(*args)


def head_block_copies(ids_ref, head_ref, buf, sems, rels, cols):
    copies = []
    for k, rel in enumerate(rels):
        start = pl.multiple_of((ids_ref[1] ^ rel) * cols, cols)
        copies.append(
            pltpu.make_async_copy(head_ref.at[pl.ds(start, cols), :], buf.at[k], sems.at[k])
        )
    for copy in copies:
        copy.start()
    return copies


def project_first(rels, ids_ref, head_ref, *refs):
    blocks, (acc_ref, buf, sems) = refs[: len(rels)], refs[len(rels) :]
    copies = head_block_copies(ids_ref, head_ref, buf, sems, rels, acc_ref.shape[1])
    for k, block in enumerate(blocks):
        copies[k].wait()
        part = dot(block[...], buf[k], 1, 0)
        acc_ref[...] = part if k == 0 else acc_ref[...] + part


def project_last(rels, ids_ref, head_ref, *refs):
    blocks = refs[: len(rels)]
    acc_ref, count_ref, loss_ref, send_ref, out_ref, buf, sems = refs[len(rels) :]
    rows, cols = acc_ref.shape
    copies = head_block_copies(ids_ref, head_ref, buf, sems, rels, cols)
    total = acc_ref[...]
    for k, block in enumerate(blocks):
        copies[k].wait()
        total = total + dot(block[...], buf[k], 1, 0)
    proj = total.astype(BF)
    lanes = out_ref.shape[1]
    for c in range(cols // lanes):
        out_ref[c * rows : (c + 1) * rows, :] = proj[:, c * lanes : (c + 1) * lanes]
    base = cols // lanes * rows
    queries = count_ref.shape[0]
    out_ref[base : base + queries, :] = count_ref[...].astype(BF)
    loss = loss_ref[...]
    high = loss.astype(BF).astype(F32)
    middle = (loss - high).astype(BF).astype(F32)
    low = loss - high - middle
    top = high + pltpu.roll(middle, lanes // 2, 1)
    bottom = jnp.where(iota(low.shape, 0) == 7, send_ref[...].astype(F32), low)
    out_ref[base + queries : base + queries + 16, :] = jnp.concatenate([top, bottom], 0).astype(BF)


def score_own(n, fetch_block, ids_ref, *refs):
    packs = refs[:n]
    t_ref, q_ref, d_ref, fetched_ref, idx_ref, count_ref, loss_ref, send_ref, pos_ref = refs[n:]
    queries, slots = count_ref.shape[1:]
    cols = q_ref.shape[2]
    lanes = slots
    base = cols // lanes * 2 * queries
    send_ref[...] = jnp.zeros(send_ref.shape, jnp.int32)
    for e in range(n):
        pack = packs[e]
        for c in range(cols // lanes):
            low = c * 2 * queries
            q_ref[e, :, c * lanes : (c + 1) * lanes] = pack[low : low + queries, :]
            d_ref[e * queries : (e + 1) * queries, c * lanes : (c + 1) * lanes] = pack[
                low + queries : low + 2 * queries, :
            ]
        count_ref[e] = pack[base : base + queries, :].astype(F32)
        misc = pack[base + queries : base + queries + 16, :].astype(F32)
        top, bottom = misc[0:8, :], misc[8:16, :]
        bottom_loss = jnp.where(iota(bottom.shape, 1) < lanes // 2, bottom, 0.0)
        wide = top + pltpu.roll(top, lanes // 2, 1) + bottom_loss
        loss_ref[e] = jnp.where(
            (iota(wide.shape, 0) < NW) & (iota(wide.shape, 1) < queries), wide, 0.0
        )
        sent = bottom[7:8, :].astype(jnp.int32)
        send_ref[e : e + 1, :] = jnp.where(sent < 0, 0, sent + (e * queries + 1))
    me = ids_ref[0]
    pad_rows = send_ref.shape[0]
    sub, lane = iota((pad_rows, slots), 0), iota((pad_rows, slots), 1)
    doc_ids = iota((n * queries, slots), 0) + 1
    eye = iota((queries, queries), 0) == iota((queries, queries), 1)
    pos_ref[...] = jnp.zeros(pos_ref.shape, F32)

    def owner(r, carry):
        table = send_ref[...]
        found = jnp.zeros((pad_rows, slots), jnp.int32)
        for e in range(n):
            sender = me ^ e
            shift = lax.rem((sender - (me ^ r)) * fetch_block + slots, slots)
            rolled = pltpu.roll(table, shift, 1)
            found = jnp.where((sub == e) & (lane // fetch_block == sender), rolled, found)
        row = jnp.sum(found, axis=0, keepdims=True)
        idx_ref[:, pl.ds(pl.multiple_of(r * slots, slots), slots)] = jnp.broadcast_to(
            row, (8, slots)
        )
        select = (doc_ids == row).astype(F32).astype(BF)
        fetched = dot(select, d_ref[...], 0, 0).astype(BF)
        fetched_ref[r] = fetched
        query = q_ref[r]
        start = pl.multiple_of(r * queries, queries)
        t_ref[pl.ds(start, queries), :] = dot(query, fetched, 1, 1)
        pairs = dot(query, d_ref[pl.ds(start, queries), :], 1, 1)
        pos_ref[pl.ds(r, 1), 0:queries] = jnp.sum(jnp.where(eye, pairs, 0.0), axis=0, keepdims=True)
        return carry

    lax.fori_loop(0, n, owner, 0)
    t_ref[n * queries :, :] = pos_ref[...]


def add_arrays(a_ref, b_ref, out_ref):
    out_ref[...] = a_ref[...] + b_ref[...]


def column(row, queries):
    lanes = row.shape[1]
    eye = iota((queries, lanes), 0) == iota((queries, lanes), 1)
    return jnp.sum(jnp.where(eye, row, 0.0), axis=1, keepdims=True)


def width_grad(neg, pos, count, loss, scale, weight):
    named = count > 0.0
    neg_logit = neg * scale
    pos_logit = pos * scale
    highest = jnp.max(jnp.where(named, neg_logit, -jnp.inf), axis=1, keepdims=True)
    highest = jnp.maximum(highest, pos_logit)
    neg_exp = jnp.where(named, count * jnp.exp(neg_logit - highest), 0.0)
    pos_exp = jnp.exp(pos_logit - highest)
    inverse = 1.0 / (jnp.sum(neg_exp, axis=1, keepdims=True) + pos_exp)
    row_weight = loss * weight
    return neg_exp * (row_weight * inverse), row_weight * (pos_exp * inverse - 1.0)


def inner_widths(n, bounds, ids_ref, scale_ref, t_ref, q_ref, d_ref, f_ref, count_ref, loss_ref, *outs):
    seg_ref, col_ref = outs
    inner = len(bounds) - 1
    queries, slots = count_ref.shape[1:]
    cols = q_ref.shape[2]
    eye = iota((queries, queries), 0) == iota((queries, queries), 1)
    eye_wide = (iota((queries, slots), 0) == iota((queries, slots), 1)).astype(F32)
    reach = [-(-bound // 128) * 128 for bound in bounds[1:]]
    masks = [
        (iota((1, reach[w]), 1) < bounds[w + 1]).astype(F32).astype(BF) for w in range(inner - 1)
    ]

    def owner(r, carry):
        start = pl.multiple_of(r * queries, queries)
        count = count_ref[r]
        loss_cols = dot(eye_wide, loss_ref[r], 1, 1, HI)
        col_ref[r, :, 0:8] = loss_cols
        neg_sum, pos_sum = None, None
        for w in reversed(range(inner)):
            if w == inner - 1:
                neg = t_ref[pl.ds(start, queries), :]
                pos = column(t_ref[pl.ds(n * queries + r, 1), :], queries)
            else:
                query = q_ref[r, :, 0 : reach[w]] * masks[w]
                neg = dot(query, f_ref[r, :, 0 : reach[w]], 1, 1)
                pairs = dot(query, d_ref[pl.ds(start, queries), 0 : reach[w]], 1, 1)
                pos = jnp.sum(jnp.where(eye, pairs, 0.0), axis=1, keepdims=True)
            neg_grad, pos_grad = width_grad(
                neg, pos, count, loss_cols[:, w : w + 1], scale_ref[0, w], scale_ref[1, w]
            )
            neg_sum = neg_grad if neg_sum is None else neg_sum + neg_grad
            pos_sum = pos_grad if pos_sum is None else pos_sum + pos_grad
            seg_ref[w, pl.ds(start, queries), :] = neg_sum
            col_ref[r, :, 8 + w : 9 + w] = pos_sum
        return carry

    lax.fori_loop(0, n, owner, 0)


def gradients(n, bounds, steps, ids_ref, scale_ref, head_ref, *refs):
    first = min(1, steps - 1)
    sums = refs[: steps + 1 - first]
    q_ref, d_ref, f_ref, idx_ref, count_ref, seg_ref, col_ref = refs[len(sums) : len(sums) + 7]
    g_ref, keep_ref, give_ref, back_ref, pos_ref, head_buf, sem = refs[len(sums) + 7 :]
    inner = len(bounds) - 1
    queries, slots = count_ref.shape[1:]
    cols = q_ref.shape[2]
    fetch = pltpu.make_async_copy(head_ref, head_buf, sem)
    fetch.start()
    lane = iota((1, cols), 1)
    inside = [(lane >= bounds[s]) & (lane < bounds[s + 1]) for s in range(inner)]
    masks = [m.astype(F32).astype(BF) for m in inside]

    def by_column(columns):
        wide = jnp.zeros((queries, cols), F32)
        for s in range(inner):
            wide = jnp.where(inside[s], columns[:, s : s + 1], wide)
        return wide

    def owner(r, carry):
        start = pl.multiple_of(r * queries, queries)
        count = count_ref[r]
        columns = col_ref[r]
        neg_sum, pos_sum = None, None
        for step in range(1, steps + 1):
            w = inner - 1 + step
            used = sums[step - first : step - first + 1] if step < steps else sums[-2:]
            neg = sum(ref[pl.ds(start, queries), :] for ref in used)
            pos = sum(ref[pl.ds(n * queries + r, 1), :] for ref in used)
            neg_grad, pos_grad = width_grad(
                neg,
                column(pos, queries),
                count,
                columns[:, w : w + 1],
                scale_ref[0, w],
                scale_ref[1, w],
            )
            neg_sum = neg_grad if neg_sum is None else neg_sum + neg_grad
            pos_sum = pos_grad if pos_sum is None else pos_sum + pos_grad
        stacked = jnp.concatenate(
            [(seg_ref[s, pl.ds(start, queries), :] + neg_sum).astype(BF) for s in range(inner)], 0
        )
        pos_seg = columns[:, 8 : 8 + inner] + pos_sum
        pos_ref[r, :, 0:inner] = pos_seg
        query = q_ref[r]
        levels = dot(stacked, f_ref[r], 1, 0)
        grad_query = by_column(pos_seg) * d_ref[pl.ds(start, queries), :].astype(F32)
        for s in range(inner):
            grad_query += jnp.where(inside[s], levels[s * queries : (s + 1) * queries, :], 0.0)
        g_ref[r, 0:queries, :] = grad_query.astype(BF)
        spread = jnp.concatenate([query * masks[s] for s in range(inner)], axis=0)
        back = dot(stacked, spread, 0, 0)
        back_ref[pl.ds(pl.multiple_of(r * slots, slots), slots), :] = back.astype(BF)
        return carry

    lax.fori_loop(0, n, owner, 0)

    def documents(e, carry):
        doc_ids = iota((queries, n * slots), 0) + (e * queries + 1)
        select = (doc_ids == idx_ref[0:1, :]).astype(F32).astype(BF)
        grad_doc = dot(select, back_ref[...], 1, 0)
        grad_doc += by_column(pos_ref[e, :, 0:inner]) * q_ref[e].astype(F32)
        g_ref[e, queries : 2 * queries, :] = grad_doc.astype(BF)
        return carry

    lax.fori_loop(0, n, documents, 0)
    fetch.wait()
    own = g_ref[0]
    groups = head_ref.shape[0] // cols
    for rel in range(groups):
        rows = pl.multiple_of((ids_ref[1] ^ rel) * cols, cols)
        part = dot(own, head_buf[pl.ds(rows, cols), :], 1, 1)
        if rel % 2 == 0:
            keep_ref[rel // 2] = part
        else:
            give_ref[rel // 2] = part.astype(BF)


def pick_rows(n, ids_ref, *refs):
    blocks, (even_ref, odd_ref, whole) = refs[:-3], refs[-3:]
    groups = len(blocks)
    queries = even_ref.shape[1]
    cols = blocks[0].shape[1]
    width = even_ref.shape[2]
    half = ids_ref[1] & 1
    low = pl.multiple_of(half * queries, queries)
    for rel, block in enumerate(blocks):
        whole[ids_ref[1] ^ rel] = block[pl.ds(low, queries), :]
    per = n // groups
    for e in range(n):
        owner = ids_ref[0] ^ e
        rows = whole[lax.div(owner, per)].astype(F32)
        place = lax.rem(owner, per)
        picked = rows[:, 0:width]
        for p in range(1, per):
            picked = jnp.where(place == p, rows[:, p * width : (p + 1) * width], picked)
        target = even_ref if e % 2 == 0 else odd_ref
        target[e // 2] = picked.astype(BF)


def head_tile(n, ids_ref, g_ref, own_ref, other_ref, out_ref):
    half = ids_ref[1] & 1
    queries = own_ref.shape[1]
    width = own_ref.shape[2]
    cols = g_ref.shape[2]
    mine = pl.multiple_of(half * queries, queries)
    rest = pl.multiple_of((1 - half) * queries, queries)
    rows = n * queries
    first = g_ref[:, pl.ds(mine, queries), :].reshape(rows, cols)
    second = g_ref[:, pl.ds(rest, queries), :].reshape(rows, cols)
    total = dot(own_ref[...].reshape(rows, width), first, 0, 0)
    out_ref[...] = total + dot(other_ref[...].reshape(rows, width), second, 0, 0)


def on_device(n, groups, query_rows, doc_rows, head, logit_scale, loss_grad, shortlist, send_rows):
    queries, slots = shortlist.shape
    cols = head.shape[1]
    features = head.shape[0]
    fetch_block = send_rows.shape[1] // n
    widths = [features // 2 ** (NW - 1 - w) for w in range(NW)]
    steps = groups.bit_length() - 1
    inner = NW - steps
    bounds = [0] + widths[:inner]
    sds = jax.ShapeDtypeStruct

    def swap(x, axis, size, distance):
        return lax.ppermute(x, axis, [(i, i ^ distance) for i in range(size)])

    over_mp = functools.partial(swap, axis="mp", size=groups)
    over_dp = functools.partial(swap, axis="dp", size=n)
    ids = jnp.stack([lax.axis_index("dp"), lax.axis_index("mp")]).astype(jnp.int32)
    own = jnp.concatenate([query_rows, doc_rows], axis=0)
    blocks = {0: own}
    for rel in range(1, groups):
        top = 1 << (rel.bit_length() - 1)
        source = own if rel == top else blocks[top]
        blocks[rel] = over_mp(source, distance=rel if rel == top else rel - top)
    scale = logit_scale / jnp.sqrt(jnp.array(widths, F32))
    active = jnp.array(widths, jnp.int32) > ids[1] * cols
    scales = jnp.stack([scale, jnp.where(active, scale, 0.0)])
    count = jnp.sum(
        (shortlist[:, None, :] == jnp.arange(slots, dtype=jnp.int32)[None, :, None]).astype(F32), -1
    )
    loss = jnp.pad(loss_grad.T, ((0, 8 - NW), (0, slots - queries)))

    split = max(groups // 2, 1)
    early, late = list(range(split)), list(range(split, groups))
    acc = call(
        functools.partial(project_first, early),
        sds((2 * queries, cols), F32),
        [SMEM, ANY] + [VMEM] * len(early),
        [pltpu.VMEM((len(early), cols, cols), BF), pltpu.SemaphoreType.DMA((len(early),))],
        [ids, head] + [blocks[k] for k in early],
        "project_first",
    )
    pack_rows = cols // slots * 2 * queries + queries + 16
    pack = call(
        functools.partial(project_last, late),
        sds((pack_rows, slots), BF),
        [SMEM, ANY] + [VMEM] * (len(late) + 4),
        [pltpu.VMEM((len(late), cols, cols), BF), pltpu.SemaphoreType.DMA((len(late),))],
        [ids, head] + [blocks[k] for k in late] + [acc, count, loss, send_rows],
        "project_last",
    )
    packs = {0: pack, 1: over_dp(pack, distance=1)}
    for k in range(1, n // 2):
        packs[2 * k] = over_dp(pack, distance=2 * k)
    for k in range(1, n // 2):
        packs[2 * k + 1] = over_dp(packs[2 * k], distance=1)

    pos_rows = -(-n // 8) * 8
    total, q_all, d_all, fetched, idx, counts, losses = call(
        functools.partial(score_own, n, fetch_block),
        (
            sds((n * queries + pos_rows, slots), F32),
            sds((n, queries, cols), BF),
            sds((n * queries, cols), BF),
            sds((n, slots, cols), BF),
            sds((8, n * slots), jnp.int32),
            sds((n, queries, slots), F32),
            sds((n, 8, slots), F32),
        ),
        [SMEM] + [VMEM] * n,
        [pltpu.VMEM((pos_rows, slots), jnp.int32), pltpu.VMEM((pos_rows, slots), F32)],
        [ids] + [packs[e] for e in range(n)],
        "score_own",
    )
    levels = [total]
    for step in range(steps):
        received = over_mp(levels[-1], distance=1 << step)
        if step < steps - 1:
            pair = [levels[-1], received]
            levels.append(call(add_arrays, sds(total.shape, F32), [VMEM] * 2, [], pair, "add"))
    sums = levels[min(1, steps - 1) :] + [received]
    seg, columns = call(
        functools.partial(inner_widths, n, bounds),
        (sds((inner, n * queries, slots), F32), sds((n, queries, slots), F32)),
        [SMEM, SMEM] + [VMEM] * 6,
        [],
        [ids, scales, total, q_all, d_all, fetched, counts, losses],
        "inner_widths",
    )

    even, odd = call(
        functools.partial(pick_rows, n),
        (sds((n // 2, queries, features // n), BF),) * 2,
        [SMEM] + [VMEM] * groups,
        [pltpu.VMEM((groups, queries, cols), BF)],
        [ids] + [blocks[k] for k in range(groups)],
        "pick_rows",
    )
    ready = jnp.stack([even, over_dp(odd, distance=1)], axis=1)
    rows = [ready[0]] + [over_dp(ready[k], distance=2 * k) for k in range(1, n // 2)]
    own_rows = jnp.stack(rows).reshape(n, queries, features // n)
    other_rows = over_mp(own_rows, distance=1)

    grads, keep, give = call(
        functools.partial(gradients, n, bounds, steps),
        (
            sds((n, 2 * queries, cols), BF),
            sds((groups // 2, 2 * queries, cols), F32),
            sds((groups // 2, 2 * queries, cols), BF),
        ),
        [SMEM, SMEM, ANY] + [VMEM] * (len(sums) + 7),
        [
            pltpu.VMEM((n * slots, cols), BF),
            pltpu.VMEM((n, queries, slots), F32),
            pltpu.VMEM(head.shape, BF),
            pltpu.SemaphoreType.DMA,
        ],
        [ids, scales, head] + sums + [q_all, d_all, fetched, idx, counts, seg, columns],
        "gradients",
    )
    for step in range(steps):
        got = over_mp(give, distance=1 << step).astype(F32)
        whole = keep + got
        if step < steps - 1:
            keep, give = whole[0::2], whole[1::2].astype(BF)
    out = whole[0].astype(BF)
    head_grad = call(
        functools.partial(head_tile, n),
        sds((features // n, cols), F32),
        [SMEM] + [VMEM] * 3,
        [],
        [ids, grads, own_rows, other_rows],
        "head_tile",
    )
    return out[:queries], out[queries:], head_grad


def solution(mesh):
    placed = (
        P("dp", "mp"),
        P("dp", "mp"),
        P(None, "mp"),
        P(),
        P("dp", None),
        P("dp", None),
        P("dp", None),
    )
    return jax.shard_map(
        functools.partial(on_device, mesh.shape["dp"], mesh.shape["mp"]),
        mesh=mesh,
        in_specs=placed,
        out_specs=(P("dp", "mp"), P("dp", "mp"), P("dp", "mp")),
        check_vma=False,
    )
```
